32 devices in a mesh: dp: 1 (over z), y: 4 (over y), x: 8 (over x, core).
Axes of the slice: x: 4, y: 4, z: 1, core: 2. Of those that a mesh axis runs over, the one named last changes fastest.
The devices are a block of a 4x4x8 slice.
Arguments:
- hidden: bfloat16 [256, 4096], P('dp', ('x', 'y'))
- ln1_gain: bfloat16 [4096], P(('x', 'y'))
- ln1_bias: bfloat16 [4096], P(('x', 'y'))
- w_qkv: bfloat16 [4096, 3, 32, 128], P('x', None, 'y')
- b_qkv: bfloat16 [3, 32, 128], P(None, ('y', 'x'))
- w_out: bfloat16 [32, 128, 4096], P('y', None, 'x')
- b_out: bfloat16 [4096], P(('x', 'y'))
- ln2_gain: bfloat16 [4096], P(('x', 'y'))
- ln2_bias: bfloat16 [4096], P(('x', 'y'))
- w_up: bfloat16 [4096, 16384], P('x', 'y')
- b_up: bfloat16 [16384], P(('y', 'x'))
- w_down: bfloat16 [16384, 4096], P('y', 'x')
- b_down: bfloat16 [4096], P(('x', 'y'))
- k_cache: bfloat16 [256, 256, 32, 128], P('dp', None, ('y', 'x'))
- v_cache: bfloat16 [256, 256, 32, 128], P('dp', None, ('y', 'x'))
- q_pos: int32 [256], P('dp')
- k_pos: int32 [256, 256], P('dp')
- k_valid: int32 [256, 256], P('dp')
Outputs:
- output 1: bfloat16 [256, 4096], P('dp', ('x', 'y'))
- output 2: bfloat16 [256, 32, 128], P('dp', ('y', 'x'))
- output 3: bfloat16 [256, 32, 128], P('dp', ('y', 'x'))
All inputs are finite; a program needn't handle non-finite values.
Results may differ from the reference program's by a relative error of at most 0.0129273.
Values are sent between devices in bfloat16 or wider.
A program may use at most 768 MiB of HBM per device.

```python
import math
import jax
import jax.numpy as jnp
from jax import lax

HID = 4096
HEADS = 32
HEAD = 128
FF = 16384
BATCH = 256
CTX = 256
XS = 8
YS = 4
TOKEN_GROUP = 8
EPS = 1e-5


def alibi_slopes(num_heads):
    closest = 2 ** int(math.floor(math.log2(num_heads)))
    base_part = [2.0 ** (-8.0 * (index + 1) / closest) for index in range(closest)]
    extra_part = [2.0 ** (-4.0 * (2 * index + 1) / closest) for index in range(num_heads - closest)]
    return jnp.array(base_part + extra_part, dtype=jnp.float32)


def setup_inputs(seed: int = 0, part: int = 0) -> dict:
    key = jax.random.key(seed)
    weight_keys = jax.random.split(key, 12)
    w_qkv = (jax.random.normal(weight_keys[0], (HID, 3, HEADS, HEAD), jnp.float32) * HID ** -0.5).astype(jnp.bfloat16)
    b_qkv = (0.3 * jax.random.normal(weight_keys[1], (3, HEADS, HEAD), jnp.float32)).astype(jnp.bfloat16)
    w_out = (jax.random.normal(weight_keys[2], (HEADS, HEAD, HID), jnp.float32) * HID ** -0.5).astype(jnp.bfloat16)
    b_out = (0.3 * jax.random.normal(weight_keys[3], (HID,), jnp.float32)).astype(jnp.bfloat16)
    w_up = (jax.random.normal(weight_keys[4], (HID, FF), jnp.float32) * HID ** -0.5).astype(jnp.bfloat16)
    b_up = (0.3 * jax.random.normal(weight_keys[5], (FF,), jnp.float32)).astype(jnp.bfloat16)
    w_down = (jax.random.normal(weight_keys[6], (FF, HID), jnp.float32) * FF ** -0.5).astype(jnp.bfloat16)
    b_down = (0.3 * jax.random.normal(weight_keys[7], (HID,), jnp.float32)).astype(jnp.bfloat16)
    ln1_gain = (0.6 + 0.8 * jax.random.uniform(weight_keys[8], (HID,), jnp.float32)).astype(jnp.bfloat16)
    ln1_bias = (0.3 * jax.random.normal(weight_keys[9], (HID,), jnp.float32)).astype(jnp.bfloat16)
    ln2_gain = (0.6 + 0.8 * jax.random.uniform(weight_keys[10], (HID,), jnp.float32)).astype(jnp.bfloat16)
    ln2_bias = (0.3 * jax.random.normal(weight_keys[11], (HID,), jnp.float32)).astype(jnp.bfloat16)
    part_keys = jax.random.split(jax.random.fold_in(key, part), 8)
    col_scale = 0.5 + 1.5 * jax.random.uniform(part_keys[0], (HID,), jnp.float32)
    col_shift = 0.5 * jax.random.normal(part_keys[1], (HID,), jnp.float32)
    row_shift = 0.3 * jax.random.normal(part_keys[2], (BATCH, 1), jnp.float32)
    hidden = (jax.random.normal(part_keys[3], (BATCH, HID), jnp.float32) * col_scale + col_shift + row_shift).astype(jnp.bfloat16)
    k_cache = jax.random.normal(part_keys[4], (BATCH, CTX, HEADS, HEAD), jnp.float32).astype(jnp.bfloat16)
    v_cache = jax.random.normal(part_keys[5], (BATCH, CTX, HEADS, HEAD), jnp.float32).astype(jnp.bfloat16)
    q_pos = jax.random.randint(part_keys[6], (BATCH,), CTX, 8 * CTX, dtype=jnp.int32)
    slot_index = jnp.arange(CTX, dtype=jnp.int32)
    k_pos = q_pos[:, None] - CTX + (slot_index[None, :] - q_pos[:, None]) % CTX
    k_valid = (jax.random.randint(part_keys[7], (BATCH, CTX), 0, 4, dtype=jnp.int32) > 0).astype(jnp.int32)
    return {"hidden": hidden, "ln1_gain": ln1_gain, "ln1_bias": ln1_bias, "w_qkv": w_qkv, "b_qkv": b_qkv, "w_out": w_out, "b_out": b_out, "ln2_gain": ln2_gain, "ln2_bias": ln2_bias, "w_up": w_up, "b_up": b_up, "w_down": w_down, "b_down": b_down, "k_cache": k_cache, "v_cache": v_cache, "q_pos": q_pos, "k_pos": k_pos, "k_valid": k_valid}


def layer_norm(rows, gain, shift):
    rows_f32 = rows.astype(jnp.float32)
    mean = jnp.sum(rows_f32, axis=1, keepdims=True) / HID
    variance = jnp.sum(rows_f32 * rows_f32, axis=1, keepdims=True) / HID - mean * mean
    return ((rows_f32 - mean) * lax.rsqrt(variance + EPS) * gain.astype(jnp.float32) + shift.astype(jnp.float32)).astype(jnp.bfloat16)


def block_sum(left, right, blocks):
    width = left.shape[1] // blocks
    partials = [jnp.dot(left[:, block * width:(block + 1) * width], right[block * width:(block + 1) * width], preferred_element_type=jnp.float32).astype(jnp.bfloat16).astype(jnp.float32) for block in range(blocks)]
    return sum(partials).astype(jnp.bfloat16)


def reference(hidden, ln1_gain, ln1_bias, w_qkv, b_qkv, w_out, b_out, ln2_gain, ln2_bias, w_up, b_up, w_down, b_down, k_cache, v_cache, q_pos, k_pos, k_valid):
    slopes = alibi_slopes(HEADS)
    score_scale = 1.0 / math.sqrt(HEAD)
    normed = layer_norm(hidden, ln1_gain, ln1_bias)
    qkv_sum = block_sum(normed, w_qkv.reshape(HID, 3 * HEADS * HEAD), XS)
    qkv_heads = (qkv_sum.astype(jnp.float32) + b_qkv.reshape(1, 3 * HEADS * HEAD).astype(jnp.float32)).astype(jnp.bfloat16).reshape(BATCH, 3, HEADS, HEAD)
    query = qkv_heads[:, 0]
    key_new = qkv_heads[:, 1]
    val_new = qkv_heads[:, 2]

    def attend(group):
        grp_query, grp_key, grp_val, grp_kcache, grp_vcache, grp_qpos, grp_kpos, grp_valid = group
        query_f32 = grp_query.astype(jnp.float32)
        scores = jnp.einsum("bnd,btnd->bnt", query_f32, grp_kcache.astype(jnp.float32)) * score_scale
        distance = (grp_qpos[:, None] - grp_kpos).astype(jnp.float32)
        scores = scores - slopes[None, :, None] * distance[:, None, :]
        scores = jnp.where(grp_valid[:, None, :] > 0, scores, -1e30)
        self_score = jnp.sum(query_f32 * grp_key.astype(jnp.float32), axis=2) * score_scale
        row_max = jnp.maximum(jnp.max(scores, axis=2), self_score)
        exp_scores = jnp.exp(scores - row_max[:, :, None])
        self_exp = jnp.exp(self_score - row_max)
        denominator = jnp.sum(exp_scores, axis=2) + self_exp
        weighted = jnp.einsum("bnt,btnd->bnd", exp_scores.astype(jnp.bfloat16).astype(jnp.float32), grp_vcache.astype(jnp.float32))
        weighted = weighted + self_exp.astype(jnp.bfloat16).astype(jnp.float32)[:, :, None] * grp_val.astype(jnp.float32)
        return (weighted / denominator[:, :, None]).astype(jnp.bfloat16)

    groups = BATCH // TOKEN_GROUP

    def regroup(array_in):
        return array_in.reshape((groups, TOKEN_GROUP) + array_in.shape[1:])

    attended = lax.map(attend, (regroup(query), regroup(key_new), regroup(val_new), regroup(k_cache), regroup(v_cache), regroup(q_pos), regroup(k_pos), regroup(k_valid)))
    attended = attended.reshape(BATCH, HEADS * HEAD)
    attn_sum = block_sum(attended, w_out.reshape(HEADS * HEAD, HID), YS)
    residual = (hidden.astype(jnp.float32) + attn_sum.astype(jnp.float32) + b_out.astype(jnp.float32)).astype(jnp.bfloat16)
    normed_mlp = layer_norm(residual, ln2_gain, ln2_bias)
    up_sum = block_sum(normed_mlp, w_up, XS)
    activated = jax.nn.gelu(up_sum.astype(jnp.float32) + b_up.astype(jnp.float32), approximate=True).astype(jnp.bfloat16)
    down_sum = block_sum(activated, w_down, YS)
    result = (residual.astype(jnp.float32) + down_sum.astype(jnp.float32) + b_down.astype(jnp.float32)).astype(jnp.bfloat16)
    return (result, key_new, val_new)
```

```python
import functools
import math
import jax
import jax.numpy as jnp
from jax import lax
from jax.experimental import pallas as pl
from jax.experimental.pallas import tpu as pltpu
from jax.sharding import PartitionSpec as P

EPS = 1e-5
CORES = 2
MESH = pl.DeviceIdType.MESH
F32 = jnp.float32
BF16 = jnp.bfloat16


def alibi_slopes(num_heads):
    closest = 2 ** int(math.floor(math.log2(num_heads)))
    base_part = [2.0 ** (-8.0 * (index + 1) / closest) for index in range(closest)]
    extra_part = [2.0 ** (-4.0 * (2 * index + 1) / closest) for index in range(num_heads - closest)]
    return base_part + extra_part


def dot(left, right):
    return jnp.dot(left, right, preferred_element_type=F32)


class Links:
    def __init__(self, send_sems, recv_sems):
        self.send_sems, self.recv_sems = send_sems, recv_sems
        self.used = 0
        self.started = []

    def send(self, src, dst, device):
        copy = pltpu.make_async_remote_copy(
            src_ref=src, dst_ref=dst, send_sem=self.send_sems.at[self.used], recv_sem=self.recv_sems.at[self.used],
            device_id=device, device_id_type=MESH)
        self.used += 1
        copy.start()
        self.started.append(copy)
        return copy

    def drain(self):
        for copy in self.started:
            copy.wait_send()
        self.started = []


class RingSum:
    def __init__(self, links, own, travel, landed, up, down, pos, count):
        self.links, self.own, self.travel, self.landed = links, own, travel, landed
        self.up, self.down, self.pos = up, down, pos
        self.ahead, self.behind, self.far = lax.rem(pos + 1, count), lax.rem(pos + count - 1, count), lax.rem(pos + 2, count)

    def push(self, slot, value, device):
        self.travel[slot] = value.astype(BF16)
        return self.links.send(self.travel.at[slot], self.landed.at[slot], device)

    def first_far(self):
        self.far_a = self.push(0, self.own(self.far, 0), self.up)
        self.far_b = self.push(1, self.own(self.far, 1), self.down)

    def first_near(self):
        self.near_b = self.push(2, self.own(self.ahead, 1), self.up)
        self.near_a = self.push(3, self.own(self.behind, 0), self.down)

    def relay(self):
        self.far_a.wait_recv()
        self.comb_a = self.push(4, self.own(self.ahead, 0) + self.landed[0].astype(F32), self.up)
        self.far_b.wait_recv()
        self.comb_b = self.push(5, self.own(self.behind, 1) + self.landed[1].astype(F32), self.down)

    def final(self):
        self.near_a.wait_recv()
        self.comb_a.wait_recv()
        half_a = self.own(self.pos, 0) + self.landed[3].astype(F32) + self.landed[4].astype(F32)
        self.near_b.wait_recv()
        self.comb_b.wait_recv()
        half_b = self.own(self.pos, 1) + self.landed[2].astype(F32) + self.landed[5].astype(F32)
        return half_a, half_b


class RingGather:
    def __init__(self, links, buf, slot, half, up, down, pos, count, sibling=None):
        self.links, self.buf, self.slot, self.half, self.up, self.down = links, buf, slot, half, up, down
        self.pos, self.sibling = pos, sibling
        self.ahead, self.behind, self.far = lax.rem(pos + 1, count), lax.rem(pos + count - 1, count), lax.rem(pos + 2, count)
        self.sib = []

    def view(self, pos, part):
        return self.buf.at[self.slot(pos), pl.ds(part * self.half, self.half)]

    def send(self, pos, part, device):
        view = self.view(pos, part)
        return self.links.send(view, view, device)

    def cross(self, pos, part):
        if self.sibling is not None:
            self.sib.append(self.send(pos, part, self.sibling))

    def first(self):
        self.up_a = self.send(self.pos, 0, self.up)
        self.down_b = self.send(self.pos, 1, self.down)
        self.up_b = self.send(self.pos, 1, self.up)
        self.down_a = self.send(self.pos, 0, self.down)
        self.cross(self.pos, 0)
        self.cross(self.pos, 1)

    def relay(self):
        self.up_a.wait_recv()
        self.far_a = self.send(self.behind, 0, self.up)
        self.cross(self.behind, 0)
        self.down_b.wait_recv()
        self.far_b = self.send(self.ahead, 1, self.down)
        self.cross(self.ahead, 1)

    def near(self):
        self.up_b.wait_recv()
        self.cross(self.behind, 1)
        self.down_a.wait_recv()
        self.cross(self.ahead, 0)

    def last(self):
        self.far_a.wait_recv()
        self.cross(self.far, 0)
        self.far_b.wait_recv()
        self.cross(self.far, 1)

    def wait_cross(self, first, count):
        for copy in self.sib[first:first + count]:
            copy.wait_recv()


def kernel(xs, ys, slopes, hid_total,
           hidden, vecs, w_qkv, w_out, w_up, w_down, k_cache, v_cache, q_pos, k_pos, k_valid,
           out, k_new, v_new,
           kmem, vmem, wraw, wtmp, wq, wo, wu, wd, qpos_v, kpos_v, valid_v,
           xg, hg, vecg, stat1, stat2, act,
           qkv_send, qkv_sib, qkv_travel, qkv_land, qbuf,
           score, dist, mask, prob, obuf, attg,
           ysend, ytravel, yland, up_send, up_sib, up_travel, up_land, upg, dacc, dtravel, dland,
           send_sems, recv_sems, load_sems):
    x_index, y_index = lax.axis_index("x"), lax.axis_index("y")
    chips = xs // CORES
    chip, core = x_index // CORES, lax.rem(x_index, CORES)
    other = 1 - core
    rows = hidden.shape[0]
    half = rows // 2
    wide = hidden.shape[1]
    ctx = k_cache.shape[1]
    hdim = k_cache.shape[2]
    group = 16
    links = Links(send_sems, recv_sems)

    def at(x, y):
        return {"x": x, "y": y}

    sibling = at(CORES * chip + other, y_index)
    x_up = at(CORES * lax.rem(chip + 1, chips) + core, y_index)
    x_down = at(CORES * lax.rem(chip + chips - 1, chips) + core, y_index)
    y_up = at(x_index, lax.rem(y_index + 1, ys))
    y_down = at(x_index, lax.rem(y_index + ys - 1, ys))
    peers = [at(lax.rem(x_index + dx, xs), lax.rem(y_index + dy, ys)) for dy in range(ys) for dx in range(xs)][1:]

    barrier = pltpu.get_barrier_semaphore()
    for peer in peers:
        pl.semaphore_signal(barrier, inc=1, device_id=peer, device_id_type=MESH)

    loads = []

    def load(src, dst):
        copy = pltpu.make_async_copy(src, dst, load_sems.at[len(loads)])
        loads.append(copy)
        copy.start()
        return copy

    ld_x = load(hidden, xg.at[y_index])
    ld_vec = load(vecs, vecg.at[y_index])
    ld_pos = [load(q_pos, qpos_v), load(k_pos, kpos_v), load(k_valid, valid_v)]
    ld_wq = load(w_qkv, wraw)
    pieces = 8
    step = rows // pieces
    ld_k = [load(k_cache.at[pl.ds(i * step, step)], kmem.at[pl.ds(i * step, step)]) for i in range(pieces)]
    ld_v = [load(v_cache.at[pl.ds(i * step, step)], vmem.at[pl.ds(i * step, step)]) for i in range(pieces)]
    ld_wo, ld_wu, ld_wd = load(w_out, wo), load(w_up, wu), load(w_down, wd)

    lane = lax.broadcasted_iota(jnp.int32, (rows, 128), 1)

    def own_stats(piece, stat):
        piece = piece.astype(F32)
        total = jnp.sum(piece, axis=1, keepdims=True)
        squares = jnp.sum(piece * piece, axis=1, keepdims=True)
        both = jnp.where(lane == 0, total, jnp.where(lane == 1, squares, 0.0))
        stat[y_index * xs + x_index] = both.T[0:2, :]

    def send_stats(stat):
        mine = stat.at[y_index * xs + x_index]
        return [links.send(mine, mine, peer) for peer in peers]

    def normalize(stat, arrivals, buf, gain_row):
        for copy in arrivals:
            copy.wait_recv()
        total = jnp.sum(stat[...], axis=0)
        mean = total[0:1, :] / hid_total
        variance = total[1:2, :] / hid_total - mean * mean
        scale = lax.rsqrt(variance + EPS)
        sub = lax.broadcasted_iota(jnp.int32, (128, rows), 0)
        both = jnp.where(sub == 0, mean, scale).T
        mean_col, scale_col = both[:, 0:1], both[:, 1:2]
        for piece in range(ys):
            gain = vecg[piece, gain_row:gain_row + 1, :]
            shift = vecg[piece, gain_row + 1:gain_row + 2, :]
            value = (buf[piece].astype(F32) - mean_col) * scale_col * gain + shift
            act[:, piece * wide:(piece + 1) * wide] = value.astype(BF16)

    ld_x.wait()
    own_stats(xg[y_index], stat1)
    ld_vec.wait()
    pl.semaphore_wait(barrier, len(peers))

    stats = send_stats(stat1)
    gather = RingGather(links, xg, lambda pos: pos, half, y_up, y_down, y_index, ys)
    gather.first()
    vec_copies = [links.send(vecg.at[y_index], vecg.at[y_index], at(x_index, lax.rem(y_index + dy, ys))) for dy in range(1, ys)]

    ld_wq.wait()
    kblock = wtmp.shape[1] // xs

    @pl.loop(0, w_qkv.shape[0] // kblock)
    def _(block):
        start = pl.multiple_of(block * kblock, kblock)
        for c in range(3):
            wtmp[c] = wraw[pl.ds(start, kblock), c].astype(F32).reshape(kblock * xs, hdim)
        for c in range(3):
            for n in range(xs):
                part = wtmp[c, pl.ds(n, kblock, stride=xs), :].astype(BF16)
                wq[c * chips + n // CORES, pl.ds(start, kblock), (n % CORES) * hdim:(n % CORES + 1) * hdim] = part

    gather.relay()

    for copy in ld_pos:
        copy.wait()
    head = y_index * xs + x_index
    slope = jnp.float32(0.0)
    for index, value in enumerate(slopes):
        slope = jnp.where(head == index, jnp.float32(value), slope)
    dist[...] = slope * (qpos_v[...] - kpos_v[...].T).astype(F32)
    mask[...] = valid_v[...].astype(F32).T

    gather.near()
    gather.last()
    for copy in vec_copies:
        copy.wait_recv()
    normalize(stat1, stats, xg, 0)

    order = [lax.rem(chip + 2, chips), lax.rem(chip + 1, chips), lax.rem(chip + chips - 1, chips), chip]

    def qkv_product(c):
        arrivals = []
        for j in order:
            part = dot(act[...], wq[c * chips + j]).astype(BF16)
            for p in range(CORES):
                qkv_send[c, CORES * j + p] = part[:, p * hdim:(p + 1) * hdim]
            arrivals.append(links.send(qkv_send.at[c, CORES * j + other], qkv_sib.at[c, j], sibling))
        return arrivals

    def qkv_own(c):
        def own(j, part):
            view = pl.ds(part * half, half)
            return qkv_send[c, CORES * j + core, view].astype(F32) + qkv_sib[c, j, view].astype(F32)
        return own

    def qkv_ring(c):
        return RingSum(links, qkv_own(c), qkv_travel.at[c], qkv_land.at[c], x_up, x_down, chip, chips)

    def qkv_finish(ring, c):
        bias = vecg[y_index, 6 + c:7 + c, :]
        for part, value in enumerate(ring.final()):
            value = value.astype(BF16).astype(F32) + bias
            qbuf[c, part * half:(part + 1) * half, :] = value.astype(BF16)

    q_arr = qkv_product(0)
    q_ring, k_ring, v_ring = qkv_ring(0), qkv_ring(1), qkv_ring(2)
    q_arr[0].wait_recv()
    q_ring.first_far()
    for copy in q_arr[1:]:
        copy.wait_recv()
    q_ring.first_near()
    k_arr = qkv_product(1)
    q_ring.relay()
    for copy in k_arr:
        copy.wait_recv()
    k_ring.first_far()
    k_ring.first_near()
    v_arr = qkv_product(2)
    qkv_finish(q_ring, 0)

    for copy in ld_k:
        copy.wait()
    score_scale = hdim ** -0.5
    lanes = lax.broadcasted_iota(jnp.int32, (hdim, 128), 1)

    def query_t(part):
        return qbuf[0, part * half:(part + 1) * half, :].astype(F32).T

    def scores(part):
        q_t = query_t(part)
        columns = slice(part * half, (part + 1) * half)
        score[:, columns] = jnp.zeros((ctx, half), F32)

        @pl.loop(0, half // group)
        def _(block):
            base = part * half + block * group
            keys = jnp.concatenate([kmem[base + i] for i in range(group)], axis=1)
            picks = jnp.concatenate([jnp.where(lanes == block * group + i, q_t, 0.0).astype(BF16) for i in range(group)], axis=0)
            score[:, columns] += dot(keys, picks)

    scores(0)
    k_ring.relay()
    for copy in v_arr:
        copy.wait_recv()
    v_ring.first_far()
    v_ring.first_near()
    scores(1)
    qkv_finish(k_ring, 1)
    v_ring.relay()

    extras = []
    for part in range(2):
        columns = slice(part * half, (part + 1) * half)
        k_t = qbuf[1, columns, :].astype(F32).T
        self_score = jnp.sum(query_t(part) * k_t, axis=0, keepdims=True) * score_scale
        value = score[:, columns] * score_scale - dist[:, columns]
        value = jnp.where(mask[:, columns] > 0.0, value, -1e30)
        row_max = jnp.maximum(jnp.max(value, axis=0, keepdims=True), self_score)
        value = jnp.exp(value - row_max)
        self_exp = jnp.exp(self_score - row_max)
        denominator = jnp.sum(value, axis=0, keepdims=True) + self_exp
        prob[columns, :] = value.astype(BF16).astype(F32).T
        sub = lax.broadcasted_iota(jnp.int32, (128, half), 0)
        both = jnp.where(sub == 0, self_exp.astype(BF16).astype(F32), denominator).T
        extras.append((both[:, 0:1], both[:, 1:2]))

    for copy in ld_v:
        copy.wait()
    row = lax.broadcasted_iota(jnp.int32, (group, ctx), 0)

    @pl.loop(0, rows // group)
    def _(block):
        base = pl.multiple_of(block * group, group)
        weights = prob[pl.ds(base, group), :]
        picks = jnp.concatenate([jnp.where(row == i, weights, 0.0).astype(BF16) for i in range(group)], axis=1)
        values = vmem[pl.ds(base, group)].reshape(group * ctx, hdim)
        obuf[pl.ds(base, group), :] = dot(picks, values)

    qkv_finish(v_ring, 2)
    for part in range(2):
        columns = slice(part * half, (part + 1) * half)
        self_exp, denominator = extras[part]
        value = obuf[columns, :] + self_exp * qbuf[2, columns, :].astype(F32)
        attg[x_index, columns, :] = (value / denominator).astype(BF16)
    k_new[...] = qbuf[1]
    v_new[...] = qbuf[2]

    gather = RingGather(links, attg, lambda pos: CORES * pos + core, half, x_up, x_down, chip, chips, sibling)
    gather.first()
    gather.relay()
    gather.near()
    gather.last()
    gather.wait_cross(0, 8)

    ld_wo.wait()
    attended = jnp.concatenate([attg[n] for n in range(xs)], axis=1)
    for j in range(0, ys, 2):
        weights = wo[:, :, j * wide:(j + 2) * wide].reshape(xs * hdim, 2 * wide)
        part = dot(attended, weights).astype(BF16)
        ysend[j] = part[:, :wide]
        ysend[j + 1] = part[:, wide:]

    def y_own(j, part):
        return ysend[j, pl.ds(part * half, half)].astype(F32)

    ring = RingSum(links, y_own, ytravel, yland, y_up, y_down, y_index, ys)
    ring.first_far()
    ring.first_near()
    ring.relay()
    for part, value in enumerate(ring.final()):
        view = slice(part * half, (part + 1) * half)
        value = xg[y_index, view].astype(F32) + value.astype(BF16).astype(F32) + vecg[y_index, 4:5, :]
        hg[y_index, view] = value.astype(BF16)

    own_stats(hg[y_index], stat2)
    stats = send_stats(stat2)
    gather = RingGather(links, hg, lambda pos: pos, half, y_up, y_down, y_index, ys)
    gather.first()
    gather.relay()
    ld_wu.wait()
    gather.near()
    gather.last()
    normalize(stat2, stats, hg, 2)

    ff = up_send.shape[2]
    tile = 256
    up_arr = []
    for j in order:
        for p in (other, core):
            n = CORES * j + p
            for t in range(0, ff, tile):
                part = dot(act[...], wu[:, pl.ds(pl.multiple_of(n * ff + t, tile), tile)])
                up_send[n, :, t:t + tile] = part.astype(BF16)
            if p is other:
                up_arr.append(links.send(up_send.at[n], up_sib.at[j], sibling))

    def up_own(j, part):
        view = pl.ds(part * half, half)
        return up_send[CORES * j + core, view].astype(F32) + up_sib[j, view].astype(F32)

    ring = RingSum(links, up_own, up_travel, up_land, x_up, x_down, chip, chips)
    up_arr[0].wait_recv()
    ring.first_far()
    for copy in up_arr[1:]:
        copy.wait_recv()
    ring.first_near()
    ring.relay()
    bias = jnp.concatenate([vecg[y_index, 9 + i:10 + i, :] for i in range(ff // 128)], axis=1)
    for part, value in enumerate(ring.final()):
        value = jax.nn.gelu(value.astype(BF16).astype(F32) + bias, approximate=True)
        upg[x_index, part * half:(part + 1) * half, :] = value.astype(BF16)

    gather = RingGather(links, upg, lambda pos: CORES * pos + core, half, x_up, x_down, chip, chips, sibling)
    gather.first()
    ld_wd.wait()

    def down(slot, first):
        for t in range(0, dacc.shape[1], tile):
            part = dot(upg[slot], wd[pl.ds(pl.multiple_of(slot * ff, ff), ff), t:t + tile])
            if first:
                dacc[:, t:t + tile] = part
            else:
                dacc[:, t:t + tile] += part

    ahead, behind, far = gather.ahead, gather.behind, gather.far
    down(x_index, True)
    gather.wait_cross(0, 2)
    down(CORES * chip + other, False)
    gather.relay()
    gather.near()
    down(CORES * behind + core, False)
    down(CORES * ahead + core, False)
    gather.wait_cross(2, 4)
    down(CORES * behind + other, False)
    down(CORES * ahead + other, False)
    gather.last()
    down(CORES * far + core, False)
    gather.wait_cross(6, 2)
    down(CORES * far + other, False)

    for j in range(ys):
        ysend[j] = dacc[:, j * wide:(j + 1) * wide].astype(BF16)
    ring = RingSum(links, y_own, dtravel, dland, y_up, y_down, y_index, ys)
    ring.first_far()
    ring.first_near()
    ring.relay()
    for part, value in enumerate(ring.final()):
        view = slice(part * half, (part + 1) * half)
        value = hg[y_index, view].astype(F32) + value.astype(BF16).astype(F32) + vecg[y_index, 5:6, :]
        out[view, :] = value.astype(BF16)
    links.drain()


def solution(mesh):
    xs = mesh.shape["x"]
    ys = mesh.shape["y"]
    chips = xs // CORES
    hid_spec = P(("x", "y"))
    ff_spec = P(("y", "x"))
    cache_spec = P("dp", None, ("y", "x"), None)
    in_specs = (P("dp", ("x", "y")), hid_spec, hid_spec, P("x", None, "y", None), P(None, ("y", "x"), None), P("y", None, "x"), hid_spec, hid_spec, hid_spec, P("x", "y"), ff_spec, P("y", "x"), hid_spec, cache_spec, cache_spec, P("dp"), P("dp", None), P("dp", None))
    out_specs = (P("dp", ("x", "y")), P("dp", ("y", "x"), None), P("dp", ("y", "x"), None))

    def layer(hidden, ln1_gain, ln1_bias, w_qkv, b_qkv, w_out, b_out, ln2_gain, ln2_bias, w_up, b_up, w_down, b_down, k_cache, v_cache, q_pos, k_pos, k_valid):
        num_heads = k_cache.shape[2]
        hid_total = hidden.shape[1]
        slopes = alibi_slopes(num_heads)

        def device_step(hidden, ln1_gain, ln1_bias, w_qkv, b_qkv, w_out, b_out, ln2_gain, ln2_bias, w_up, b_up, w_down, b_down, k_cache, v_cache, q_pos, k_pos, k_valid):
            rows, wide = hidden.shape
            ctx, hdim = k_cache.shape[1], k_cache.shape[3]
            ff = b_up.shape[0]
            half = rows // 2
            small = [ln1_gain, ln1_bias, ln2_gain, ln2_bias, b_out, b_down]
            vecs = jnp.concatenate([v.reshape(1, wide) for v in small] + [b_qkv.reshape(3, hdim), b_up.reshape(ff // wide, wide)], axis=0)
            vecs = jnp.pad(vecs.astype(F32), ((0, -vecs.shape[0] % 8), (0, 0)))
            k_cache = k_cache.reshape(rows, ctx, hdim)
            v_cache = v_cache.reshape(rows, ctx, hdim)
            vm = pltpu.VMEM
            kblock = 64
            scratch = [
                vm(k_cache.shape, BF16), vm(v_cache.shape, BF16), vm(w_qkv.shape, BF16), vm((3, kblock * xs, hdim), F32),
                vm((3 * chips, w_qkv.shape[0], CORES * hdim), BF16), vm(w_out.shape, BF16), vm(w_up.shape, BF16), vm(w_down.shape, BF16),
                vm((1, rows), jnp.int32), vm(k_pos.shape, jnp.int32), vm(k_valid.shape, jnp.int32),
                vm((ys, rows, wide), BF16), vm((ys, rows, wide), BF16), vm((ys,) + vecs.shape, F32),
                vm((xs * ys, 2, rows), F32), vm((xs * ys, 2, rows), F32), vm((rows, ys * wide), BF16),
                vm((3, xs, rows, hdim), BF16), vm((3, chips, rows, hdim), BF16), vm((3, 6, half, hdim), BF16), vm((3, 6, half, hdim), BF16), vm((3, rows, hdim), BF16),
                vm((ctx, rows), F32), vm((ctx, rows), F32), vm((ctx, rows), F32), vm((rows, ctx), F32), vm((rows, hdim), F32), vm((xs, rows, hdim), BF16),
                vm((ys, rows, wide), BF16), vm((6, half, wide), BF16), vm((6, half, wide), BF16),
                vm((xs, rows, ff), BF16), vm((chips, rows, ff), BF16), vm((6, half, ff), BF16), vm((6, half, ff), BF16), vm((xs, rows, ff), BF16),
                vm((rows, ys * wide), F32), vm((6, half, wide), BF16), vm((6, half, wide), BF16),
                pltpu.SemaphoreType.DMA((180,)), pltpu.SemaphoreType.DMA((180,)), pltpu.SemaphoreType.DMA((32,)),
            ]
            any_spec = pl.BlockSpec(memory_space=pl.ANY)
            vm_spec = pl.BlockSpec(memory_space=pltpu.VMEM)
            out, k_new, v_new = pl.pallas_call(
                functools.partial(kernel, xs, ys, slopes, hid_total),
                out_shape=[jax.ShapeDtypeStruct((rows, wide), BF16), jax.ShapeDtypeStruct((rows, hdim), BF16), jax.ShapeDtypeStruct((rows, hdim), BF16)],
                in_specs=[any_spec] * 11,
                out_specs=[vm_spec] * 3,
                scratch_shapes=scratch,
                compiler_params=pltpu.CompilerParams(collective_id=0, has_side_effects=True, vmem_limit_bytes=67043328),
            )(hidden, vecs, w_qkv, w_out, w_up, w_down, k_cache, v_cache, q_pos.reshape(1, rows), k_pos, k_valid)
            return out, k_new.reshape(rows, 1, hdim), v_new.reshape(rows, 1, hdim)

        return jax.shard_map(device_step, mesh=mesh, in_specs=in_specs, out_specs=out_specs, check_vma=False)(hidden, ln1_gain, ln1_bias, w_qkv, b_qkv, w_out, b_out, ln2_gain, ln2_bias, w_up, b_up, w_down, b_down, k_cache, v_cache, q_pos, k_pos, k_valid)

    return layer
```

```python
import functools
import math
import jax
import jax.numpy as jnp
from jax import lax
from jax.experimental import pallas as pl
from jax.experimental.pallas import tpu as pltpu
from jax.sharding import PartitionSpec as P

EPS = 1e-5
CORES = 2
MESH = pl.DeviceIdType.MESH
F32 = jnp.float32
BF16 = jnp.bfloat16


def alibi_slopes(num_heads):
    closest = 2 ** int(math.floor(math.log2(num_heads)))
    base_part = [2.0 ** (-8.0 * (index + 1) / closest) for index in range(closest)]
    extra_part = [2.0 ** (-4.0 * (2 * index + 1) / closest) for index in range(num_heads - closest)]
    return base_part + extra_part


def dot(left, right):
    return jnp.dot(left, right, preferred_element_type=F32)


class Links:
    def __init__(self, send_sems, recv_sems):
        self.send_sems, self.recv_sems = send_sems, recv_sems
        self.used = 0
        self.started = []

    def send(self, src, dst, device):
        copy = pltpu.make_async_remote_copy(
            src_ref=src, dst_ref=dst, send_sem=self.send_sems.at[self.used], recv_sem=self.recv_sems.at[self.used],
            device_id=device, device_id_type=MESH)
        self.used += 1
        copy.start()
        self.started.append(copy)
        return copy

    def drain(self):
        for copy in self.started:
            copy.wait_send()
        self.started = []


class RingSum:
    def __init__(self, links, own, travel, landed, up, down, pos, count):
        self.links, self.own, self.travel, self.landed = links, own, travel, landed
        self.up, self.down, self.pos = up, down, pos
        self.ahead, self.behind, self.far = lax.rem(pos + 1, count), lax.rem(pos + count - 1, count), lax.rem(pos + 2, count)

    def push(self, slot, value, device):
        self.travel[slot] = value.astype(BF16)
        return self.links.send(self.travel.at[slot], self.landed.at[slot], device)

    def first_far(self):
        self.far_a = self.push(0, self.own(self.far, 0), self.up)
        self.far_b = self.push(1, self.own(self.far, 1), self.down)

    def first_near(self):
        self.near_b = self.push(2, self.own(self.ahead, 1), self.up)
        self.near_a = self.push(3, self.own(self.behind, 0), self.down)

    def relay(self):
        self.far_a.wait_recv()
        self.comb_a = self.push(4, self.own(self.ahead, 0) + self.landed[0].astype(F32), self.up)
        self.far_b.wait_recv()
        self.comb_b = self.push(5, self.own(self.behind, 1) + self.landed[1].astype(F32), self.down)

    def final(self):
        self.near_a.wait_recv()
        self.comb_a.wait_recv()
        half_a = self.own(self.pos, 0) + self.landed[3].astype(F32) + self.landed[4].astype(F32)
        self.near_b.wait_recv()
        self.comb_b.wait_recv()
        half_b = self.own(self.pos, 1) + self.landed[2].astype(F32) + self.landed[5].astype(F32)
        return half_a, half_b


class RingGather:
    def __init__(self, links, buf, slot, base, half, up, down, pos, count, sibling=None):
        self.links, self.buf, self.slot, self.base, self.half, self.up, self.down = links, buf, slot, base, half, up, down
        self.pos, self.sibling = pos, sibling
        self.ahead, self.behind, self.far = lax.rem(pos + 1, count), lax.rem(pos + count - 1, count), lax.rem(pos + 2, count)
        self.sib = []

    def view(self, pos, part):
        return self.buf.at[self.slot(pos), pl.ds(self.base + part * self.half, self.half)]

    def send(self, pos, part, device):
        view = self.view(pos, part)
        return self.links.send(view, view, device)

    def cross(self, pos, part):
        if self.sibling is not None:
            self.sib.append(self.send(pos, part, self.sibling))

    def first(self):
        self.up_a = self.send(self.pos, 0, self.up)
        self.down_b = self.send(self.pos, 1, self.down)
        self.up_b = self.send(self.pos, 1, self.up)
        self.down_a = self.send(self.pos, 0, self.down)
        self.cross(self.pos, 0)
        self.cross(self.pos, 1)

    def relay(self):
        self.up_a.wait_recv()
        self.far_a = self.send(self.behind, 0, self.up)
        self.cross(self.behind, 0)
        self.down_b.wait_recv()
        self.far_b = self.send(self.ahead, 1, self.down)
        self.cross(self.ahead, 1)

    def near(self):
        self.up_b.wait_recv()
        self.cross(self.behind, 1)
        self.down_a.wait_recv()
        self.cross(self.ahead, 0)

    def last(self):
        self.far_a.wait_recv()
        self.cross(self.far, 0)
        self.far_b.wait_recv()
        self.cross(self.far, 1)

    def wait_cross(self, first, count):
        for copy in self.sib[first:first + count]:
            copy.wait_recv()


def kernel(xs, ys, slopes, hid_total,
           hidden, ln1_gain, ln1_bias, ln2_gain, ln2_bias, b_out, b_down, b_qkv, b_up, w_qkv, w_out, w_up, w_down, k_cache, v_cache, q_pos, k_pos, k_valid,
           results,
           kmem, vmem, wraw, wtmp, wq, wo, wu, wd, qpos_v, kpos_v, valid_v,
           xg, hg, s_g1, s_b1, s_g2, s_b2, s_bo, s_bd, s_bqkv, s_bup, vecg, stat1, stat2, act,
           qkv_send, qkv_sib, qkv_travel, qkv_land, qbuf,
           score, dist, mask, prob, obuf, attg,
           ysend, ytravel, yland, up_send, up_sib, up_travel, up_land, upg, dacc, dtravel, dland,
           send_sems, recv_sems, load_sems):
    x_index, y_index = lax.axis_index("x"), lax.axis_index("y")
    chips = xs // CORES
    chip, core = x_index // CORES, lax.rem(x_index, CORES)
    other = 1 - core
    rows = hidden.shape[0]
    half = rows // 2
    wide = hidden.shape[1]
    ctx = k_cache.shape[1]
    hdim = k_cache.shape[2]
    group = 16
    links = Links(send_sems, recv_sems)

    def at(x, y):
        return {"x": x, "y": y}

    sibling = at(CORES * chip + other, y_index)
    x_up = at(CORES * lax.rem(chip + 1, chips) + core, y_index)
    x_down = at(CORES * lax.rem(chip + chips - 1, chips) + core, y_index)
    y_up = at(x_index, lax.rem(y_index + 1, ys))
    y_down = at(x_index, lax.rem(y_index + ys - 1, ys))
    peers = [at(lax.rem(x_index + dx, xs), lax.rem(y_index + dy, ys)) for dy in range(ys) for dx in range(xs)][1:]

    loads = []

    def load(src, dst):
        copy = pltpu.make_async_copy(src, dst, load_sems.at[len(loads)])
        loads.append(copy)
        copy.start()
        return copy

    ld_x = load(hidden, xg.at[y_index])
    small = [s_g1, s_b1, s_g2, s_b2, s_bo, s_bd, s_bqkv, s_bup]
    ld_vec = [load(src, dst) for src, dst in zip([ln1_gain, ln1_bias, ln2_gain, ln2_bias, b_out, b_down, b_qkv, b_up], small)]
    ld_pos = [load(q_pos, qpos_v), load(k_pos, kpos_v), load(k_valid, valid_v)]
    ld_wq = load(w_qkv, wraw)
    pieces = 8
    step = rows // pieces
    ld_k = [load(k_cache.at[pl.ds(i * step, step)], kmem.at[pl.ds(i * step, step)]) for i in range(pieces)]
    ld_v = [load(v_cache.at[pl.ds(i * step, step)], vmem.at[pl.ds(i * step, step)]) for i in range(pieces)]
    ld_wo, ld_wu, ld_wd = load(w_out, wo), load(w_up, wu), load(w_down, wd)

    barrier = pltpu.get_barrier_semaphore()
    for peer in peers:
        pl.semaphore_signal(barrier, inc=1, device_id=peer, device_id_type=MESH)

    def own_stats(piece, stat):
        lane = lax.broadcasted_iota(jnp.int32, piece.shape, 1)
        piece = piece.astype(F32)
        total = jnp.sum(piece, axis=1, keepdims=True)
        squares = jnp.sum(piece * piece, axis=1, keepdims=True)
        both = jnp.where(lane == 0, total, jnp.where(lane == 1, squares, 0.0))
        stat[y_index * xs + x_index] = both.T[0:2, :]

    def send_stats(stat):
        mine = stat.at[y_index * xs + x_index]
        return [links.send(mine, mine, peer) for peer in peers]

    def normalize(stat, arrivals, buf, base, count, gain_row):
        for copy in arrivals:
            copy.wait_recv()
        total = jnp.sum(stat[...], axis=0)
        mean = total[0:1, :] / hid_total
        variance = total[1:2, :] / hid_total - mean * mean
        scale = lax.rsqrt(variance + EPS)
        sub = lax.broadcasted_iota(jnp.int32, (128, count), 0)
        both = jnp.where(sub == 0, mean, scale).T
        mean_col, scale_col = both[:, 0:1], both[:, 1:2]
        for piece in range(ys):
            gain = vecg[piece, gain_row:gain_row + 1, :]
            shift = vecg[piece, gain_row + 1:gain_row + 2, :]
            value = (buf[piece, base:base + count].astype(F32) - mean_col) * scale_col * gain + shift
            act[base:base + count, piece * wide:(piece + 1) * wide] = value.astype(BF16)

    ld_x.wait()
    own_stats(xg[y_index], stat1)
    for copy in ld_vec:
        copy.wait()
    for index, ref in enumerate(small[:4]):
        vecg[y_index, index:index + 1, :] = ref[...].astype(F32)
    pl.semaphore_wait(barrier, len(peers))

    gather = RingGather(links, xg, lambda pos: pos, 0, half, y_up, y_down, y_index, ys)
    gather.first()
    stats = send_stats(stat1)
    vec_copies = [links.send(vecg.at[y_index], vecg.at[y_index], at(x_index, lax.rem(y_index + dy, ys))) for dy in range(1, ys)]

    ld_wq.wait()
    kblock = wtmp.shape[1] // xs

    @pl.loop(0, w_qkv.shape[0] // kblock)
    def _(block):
        start = pl.multiple_of(block * kblock, kblock)
        for c in range(3):
            wtmp[c] = wraw[pl.ds(start, kblock), c].astype(F32).reshape(kblock * xs, hdim)
        for c in range(3):
            for n in range(xs):
                part = wtmp[c, pl.ds(n, kblock, stride=xs), :].astype(BF16)
                wq[c * chips + n // CORES, pl.ds(start, kblock), (n % CORES) * hdim:(n % CORES + 1) * hdim] = part

    gather.relay()

    for copy in ld_pos:
        copy.wait()
    head = y_index * xs + x_index
    slope = jnp.float32(0.0)
    for index, value in enumerate(slopes):
        slope = jnp.where(head == index, jnp.float32(value), slope)
    dist[...] = slope * (qpos_v[...] - kpos_v[...].T).astype(F32)
    mask[...] = valid_v[...].astype(F32).T

    gather.near()
    gather.last()
    for copy in vec_copies:
        copy.wait_recv()
    normalize(stat1, stats, xg, 0, rows, 0)

    order = [lax.rem(chip + 2, chips), lax.rem(chip + 1, chips), lax.rem(chip + chips - 1, chips), chip]

    def qkv_product(c):
        arrivals = []
        for j in order:
            part = dot(act[...], wq[c * chips + j]).astype(BF16)
            for p in range(CORES):
                qkv_send[c, CORES * j + p] = part[:, p * hdim:(p + 1) * hdim]
            arrivals.append(links.send(qkv_send.at[c, CORES * j + other], qkv_sib.at[c, j], sibling))
        return arrivals

    def qkv_own(c):
        def own(j, part):
            view = pl.ds(part * half, half)
            return qkv_send[c, CORES * j + core, view].astype(F32) + qkv_sib[c, j, view].astype(F32)
        return own

    def qkv_ring(c):
        return RingSum(links, qkv_own(c), qkv_travel.at[c], qkv_land.at[c], x_up, x_down, chip, chips)

    def qkv_finish(ring, c):
        bias = s_bqkv[c:c + 1, :].astype(F32)
        for part, value in enumerate(ring.final()):
            value = value.astype(BF16).astype(F32) + bias
            if c > 0:
                results[c, part * half:(part + 1) * half, :] = value.astype(BF16)
            qbuf[c, part * half:(part + 1) * half, :] = value.astype(BF16)

    q_arr = qkv_product(0)
    q_ring, k_ring, v_ring = qkv_ring(0), qkv_ring(1), qkv_ring(2)
    q_arr[0].wait_recv()
    q_ring.first_far()
    for copy in q_arr[1:]:
        copy.wait_recv()
    q_ring.first_near()
    k_arr = qkv_product(1)
    q_ring.relay()
    for copy in k_arr:
        copy.wait_recv()
    k_ring.first_far()
    k_ring.first_near()
    v_arr = qkv_product(2)
    qkv_finish(q_ring, 0)

    for copy in ld_k:
        copy.wait()
    score_scale = hdim ** -0.5
    lanes = lax.broadcasted_iota(jnp.int32, (hdim, 128), 1)
    bundle = 2 * group

    def query_t(part):
        return qbuf[0, part * half:(part + 1) * half, :].astype(F32).T

    def scores(part, first, last):
        q_t = query_t(part)
        columns = slice(part * half, (part + 1) * half)
        if first == 0:
            score[:, columns] = jnp.zeros((ctx, half), F32)

        @pl.loop(first, last)
        def _(block):
            base = part * half + block * bundle
            keys = jnp.concatenate([kmem[base + i] for i in range(bundle)], axis=1)
            picks = jnp.concatenate([jnp.where(lanes == block * bundle + i, q_t, 0.0).astype(BF16) for i in range(bundle)], axis=0)
            score[:, columns] += dot(keys, picks)

    def softmax(part):
        columns = slice(part * half, (part + 1) * half)
        k_t = qbuf[1, columns, :].astype(F32).T
        self_score = jnp.sum(query_t(part) * k_t, axis=0, keepdims=True) * score_scale
        value = score[:, columns] * score_scale - dist[:, columns]
        value = jnp.where(mask[:, columns] > 0.0, value, -1e30)
        row_max = jnp.maximum(jnp.max(value, axis=0, keepdims=True), self_score)
        value = jnp.exp(value - row_max)
        self_exp = jnp.exp(self_score - row_max)
        denominator = jnp.sum(value, axis=0, keepdims=True) + self_exp
        prob[columns, :] = value.astype(BF16).astype(F32).T
        sub = lax.broadcasted_iota(jnp.int32, (128, half), 0)
        both = jnp.where(sub == 0, self_exp.astype(BF16).astype(F32), denominator).T
        return both[:, 0:1], both[:, 1:2]

    def weighted(part):
        row = lax.broadcasted_iota(jnp.int32, (group, ctx), 0)

        @pl.loop(part * half // group, (part + 1) * half // group)
        def _(block):
            base = pl.multiple_of(block * group, group)
            weights = prob[pl.ds(base, group), :]
            picks = jnp.concatenate([jnp.where(row == i, weights, 0.0).astype(BF16) for i in range(group)], axis=1)
            values = vmem[pl.ds(base, group)].reshape(group * ctx, hdim)
            obuf[pl.ds(base, group), :] = dot(picks, values)

    ff = up_send.shape[2]
    tile = 256
    quarter = half // 2
    blocks = half // bundle
    up_bias = jnp.concatenate([s_bup[i:i + 1, :].astype(F32) for i in range(ff // 128)], axis=1)

    def y_own(part_base):
        def own(j, part):
            return ysend[j, pl.ds(part_base + part * quarter, quarter)].astype(F32)
        return own

    def up_own(part_base):
        def own(j, part):
            view = pl.ds(part_base + part * quarter, quarter)
            return up_send[CORES * j + core, view].astype(F32) + up_sib[j, view].astype(F32)
        return own

    def x_slot(pos):
        return CORES * pos + core

    def stream(s):
        base = s * half
        mine = slice(base, base + half)

        scores(s, 0, blocks // 2)
        yield
        scores(s, blocks // 2, blocks)
        yield
        self_exp, denominator = softmax(s)
        weighted(s)
        yield
        value = obuf[mine, :] + self_exp * qbuf[2, mine, :].astype(F32)
        attg[x_index, mine, :] = (value / denominator).astype(BF16)
        gather = RingGather(links, attg, x_slot, base, quarter, x_up, x_down, chip, chips, sibling)
        gather.first()
        yield
        gather.relay()
        gather.near()
        yield
        gather.last()
        gather.wait_cross(0, 8)
        attended = jnp.concatenate([attg[n, mine] for n in range(xs)], axis=1)
        for j in range(0, ys, 2):
            weights = wo[:, :, j * wide:(j + 2) * wide].reshape(xs * hdim, 2 * wide)
            part = dot(attended, weights).astype(BF16)
            ysend[j, mine] = part[:, :wide]
            ysend[j + 1, mine] = part[:, wide:]
        ring = RingSum(links, y_own(base), ytravel.at[s], yland.at[s], y_up, y_down, y_index, ys)
        ring.first_far()
        ring.first_near()
        yield
        ring.relay()
        yield
        for part, value in enumerate(ring.final()):
            view = slice(base + part * quarter, base + (part + 1) * quarter)
            value = xg[y_index, view].astype(F32) + value.astype(BF16).astype(F32) + s_bo[...].astype(F32)
            hg[y_index, view] = value.astype(BF16)
        gather = RingGather(links, hg, lambda pos: pos, base, quarter, y_up, y_down, y_index, ys)
        own_stats(hg[y_index, mine], stat2.at[s])
        gather.first()
        stats = send_stats(stat2.at[s])
        yield
        gather.relay()
        yield
        gather.near()
        gather.last()
        normalize(stat2.at[s], stats, hg, base, half, 2)
        up_arr = []
        for j in order:
            for p in (other, core):
                n = CORES * j + p
                for t in range(0, ff, tile):
                    part = dot(act[mine, :], wu[:, pl.ds(pl.multiple_of(n * ff + t, tile), tile)])
                    up_send[n, mine, t:t + tile] = part.astype(BF16)
                if p is other:
                    up_arr.append(links.send(up_send.at[n, pl.ds(base, half)], up_sib.at[j, pl.ds(base, half)], sibling))
        yield
        ring = RingSum(links, up_own(base), up_travel.at[s], up_land.at[s], x_up, x_down, chip, chips)
        up_arr[0].wait_recv()
        ring.first_far()
        for copy in up_arr[1:]:
            copy.wait_recv()
        ring.first_near()
        yield
        ring.relay()
        yield
        for part, value in enumerate(ring.final()):
            value = jax.nn.gelu(value.astype(BF16).astype(F32) + up_bias, approximate=True)
            upg[x_index, base + part * quarter:base + (part + 1) * quarter, :] = value.astype(BF16)
        gather = RingGather(links, upg, x_slot, base, quarter, x_up, x_down, chip, chips, sibling)
        gather.first()
        yield

        def down(slot, first):
            for t in range(0, dacc.shape[1], tile):
                part = dot(upg[slot, mine], wd[pl.ds(pl.multiple_of(slot * ff, ff), ff), t:t + tile])
                if first:
                    dacc[mine, t:t + tile] = part
                else:
                    dacc[mine, t:t + tile] += part

        ahead, behind, far = gather.ahead, gather.behind, gather.far
        down(x_index, True)
        gather.wait_cross(0, 2)
        down(CORES * chip + other, False)
        yield
        gather.relay()
        gather.near()
        yield
        down(CORES * behind + core, False)
        down(CORES * ahead + core, False)
        gather.wait_cross(2, 4)
        down(CORES * behind + other, False)
        down(CORES * ahead + other, False)
        yield
        gather.last()
        down(CORES * far + core, False)
        gather.wait_cross(6, 2)
        down(CORES * far + other, False)
        for j in range(ys):
            ysend[j, mine] = dacc[mine, j * wide:(j + 1) * wide].astype(BF16)
        ring = RingSum(links, y_own(base), dtravel.at[s], dland.at[s], y_up, y_down, y_index, ys)
        ring.first_far()
        ring.first_near()
        yield
        ring.relay()
        yield
        for part, value in enumerate(ring.final()):
            view = slice(base + part * quarter, base + (part + 1) * quarter)
            value = hg[y_index, view].astype(F32) + value.astype(BF16).astype(F32) + s_bd[...].astype(F32)
            results[0, view, :] = value.astype(BF16)
        yield

    streams = [stream(0), stream(1)]

    steps = [0, 0]

    def run(*turns):
        for turn in turns:
            steps[turn] += 1
            with jax.named_scope("s%d_%02d" % (turn, steps[turn])):
                next(streams[turn])

    k_ring.relay()
    for copy in v_arr:
        copy.wait_recv()
    v_ring.first_far()
    v_ring.first_near()
    run(0)
    v_ring.relay()
    run(0)
    qkv_finish(k_ring, 1)
    for copy in ld_v:
        copy.wait()
    run(0)
    qkv_finish(v_ring, 2)
    run(0)
    run(1, 1)
    run(0)
    run(1)
    run(1)
    ld_wo.wait()
    run(0)
    run(1)
    run(0)
    run(1)
    run(0)
    run(1)
    run(0)
    run(1)
    ld_wu.wait()
    run(0)
    run(1)
    run(0)
    run(1)
    run(0)
    run(1)
    run(0)
    run(1)
    ld_wd.wait()
    run(0, 0)
    run(1)
    run(0)
    run(1)
    run(0)
    run(1)
    run(0)
    run(1)
    run(1)
    run(0)
    run(1, 1)
    links.drain()


def solution(mesh):
    xs = mesh.shape["x"]
    ys = mesh.shape["y"]
    chips = xs // CORES
    hid_spec = P(("x", "y"))
    ff_spec = P(("y", "x"))
    cache_spec = P("dp", None, ("y", "x"), None)
    in_specs = (P("dp", ("x", "y")), hid_spec, hid_spec, P("x", None, "y", None), P(None, ("y", "x"), None), P("y", None, "x"), hid_spec, hid_spec, hid_spec, P("x", "y"), ff_spec, P("y", "x"), hid_spec, cache_spec, cache_spec, P("dp"), P("dp", None), P("dp", None))
    out_specs = (P("dp", ("x", "y")), P("dp", ("y", "x"), None), P("dp", ("y", "x"), None))

    def layer(hidden, ln1_gain, ln1_bias, w_qkv, b_qkv, w_out, b_out, ln2_gain, ln2_bias, w_up, b_up, w_down, b_down, k_cache, v_cache, q_pos, k_pos, k_valid):
        num_heads = k_cache.shape[2]
        hid_total = hidden.shape[1]
        slopes = alibi_slopes(num_heads)

        def device_step(hidden, ln1_gain, ln1_bias, w_qkv, b_qkv, w_out, b_out, ln2_gain, ln2_bias, w_up, b_up, w_down, b_down, k_cache, v_cache, q_pos, k_pos, k_valid):
            rows, wide = hidden.shape
            ctx, hdim = k_cache.shape[1], k_cache.shape[3]
            ff = b_up.shape[0]
            half = rows // 2
            k_cache = k_cache.reshape(rows, ctx, hdim)
            v_cache = v_cache.reshape(rows, ctx, hdim)
            vm = pltpu.VMEM
            kblock = 64
            scratch = [
                vm(k_cache.shape, BF16), vm(v_cache.shape, BF16), vm(w_qkv.shape, BF16), vm((3, kblock * xs, hdim), F32),
                vm((3 * chips, w_qkv.shape[0], CORES * hdim), BF16), vm(w_out.shape, BF16), vm(w_up.shape, BF16), vm(w_down.shape, BF16),
                vm((1, rows), jnp.int32), vm(k_pos.shape, jnp.int32), vm(k_valid.shape, jnp.int32),
                vm((ys, rows, wide), BF16), vm((ys, rows, wide), BF16), *[vm((1, wide), BF16) for _ in range(6)], vm((3, hdim), BF16), vm((ff // wide, wide), BF16), vm((ys, 8, wide), F32),
                vm((xs * ys, 2, rows), F32), vm((2, xs * ys, 2, half), F32), vm((rows, ys * wide), BF16),
                vm((3, xs, rows, hdim), BF16), vm((3, chips, rows, hdim), BF16), vm((3, 6, half, hdim), BF16), vm((3, 6, half, hdim), BF16), vm((3, rows, hdim), BF16),
                vm((ctx, rows), F32), vm((ctx, rows), F32), vm((ctx, rows), F32), vm((rows, ctx), F32), vm((rows, hdim), F32), vm((xs, rows, hdim), BF16),
                vm((ys, rows, wide), BF16), vm((2, 6, half // 2, wide), BF16), vm((2, 6, half // 2, wide), BF16),
                vm((xs, rows, ff), BF16), vm((chips, rows, ff), BF16), vm((2, 6, half // 2, ff), BF16), vm((2, 6, half // 2, ff), BF16), vm((xs, rows, ff), BF16),
                vm((rows, ys * wide), F32), vm((2, 6, half // 2, wide), BF16), vm((2, 6, half // 2, wide), BF16),
                pltpu.SemaphoreType.DMA((280,)), pltpu.SemaphoreType.DMA((280,)), pltpu.SemaphoreType.DMA((32,)),
            ]
            any_spec = pl.BlockSpec(memory_space=pl.ANY)
            vm_spec = pl.BlockSpec(memory_space=pltpu.VMEM)
            results = pl.pallas_call(
                functools.partial(kernel, xs, ys, slopes, hid_total),
                out_shape=jax.ShapeDtypeStruct((3, rows, wide), BF16),
                in_specs=[any_spec] * 18,
                out_specs=vm_spec,
                scratch_shapes=scratch,
                compiler_params=pltpu.CompilerParams(collective_id=0, has_side_effects=True, vmem_limit_bytes=67043328),
            )(hidden, *[v.reshape(1, wide) for v in (ln1_gain, ln1_bias, ln2_gain, ln2_bias, b_out, b_down)], b_qkv.reshape(3, hdim), b_up.reshape(ff // wide, wide),
              w_qkv, w_out, w_up, w_down, k_cache, v_cache, q_pos.reshape(1, rows), k_pos, k_valid)
            out, k_new, v_new = [results[i] for i in range(3)]
            return out, k_new.reshape(rows, 1, hdim), v_new.reshape(rows, 1, hdim)

        return jax.shard_map(device_step, mesh=mesh, in_specs=in_specs, out_specs=out_specs, check_vma=False)(hidden, ln1_gain, ln1_bias, w_qkv, b_qkv, w_out, b_out, ln2_gain, ln2_bias, w_up, b_up, w_down, b_down, k_cache, v_cache, q_pos, k_pos, k_valid)

    return layer
```
